32 devices in a mesh: groups: 2 (over y), expert: 4 (over z), tensor: 4 (over x, core).
Axes of the slice: x: 2, y: 2, z: 4, core: 2. Of those that a mesh axis runs over, the one named last changes fastest.
Arguments:
- tokens: bfloat16 [2, 64, 3072], P(None, ('groups', 'expert'), 'tensor'), parts along dimension 1, may hold values from -60 to 60
- route_ids: int32 [2, 2, 64, 2], P(None, None, ('groups', 'expert')), parts along dimension 2, may hold values from 0 to 3, all different within a row; in each aligned block of 8 rows (0 to 7, 8 to 15, ..., all dimensions but the last counted through in order) at most 6 rows name the same one
- route_gates: float32 [2, 2, 64, 2], P(None, None, ('groups', 'expert')), parts along dimension 2, may hold values from 0.05 to 1
- norm_gain: float32 [2, 3072], P(None, 'tensor'), may hold values from 0.1 to 1.9
- gate_weights: bfloat16 [2, 3072, 32768], P(None, 'tensor', 'expert'), may hold values from -0.109375 to 0.109375
- up_weights: bfloat16 [2, 3072, 32768], P(None, 'tensor', 'expert'), may hold values from -0.109375 to 0.109375
- down_weights: bfloat16 [2, 32768, 3072], P(None, 'expert', 'tensor'), may hold values from -0.0625 to 0.0625
Outputs:
- layer_out: bfloat16 [2, 64, 3072], P(None, ('groups', 'expert'), 'tensor'), parts along dimension 1
The draws below stay inside these ranges and needn't reach their ends.
There are 2 independent parts, one for each index of `groups`. The reference program is written for one: setup_inputs(seed, part) draws one part's arguments, and reference() takes and returns one part's arrays. A program takes and returns all parts, laid end to end along the dimension named above; an argument that names none is the same for every part. Nothing has to cross between parts.
Inputs may be any that keep to these rules, and one draw needn't show every extreme that they name: `route_ids`: in each layer and micro-batch, the 8 tokens of one expert rank name one expert at most 6 times; in some of these blocks one expert exactly 6 times. A token's two ids differ.
All inputs are finite; a program needn't handle non-finite values.
Results may differ from the reference program's by a relative error of at most 0.0085.
Values may be sent and summed in bfloat16 or wider, within the bound.
A program may use at most 128 MiB of HBM per device.

```python
import math
import jax
import jax.numpy as jnp
import numpy as np
from jax import lax

D = 3072
EXPERT_HIDDEN = 8192
EXPERTS = 4
TOK_DEV = 8
MB = 2
LAYERS = 2
CAP = 6
GROUP = 1
TOKENS_MB = 32
N_EXPERT = 4
N_TENSOR = 4


def draw_tokens(key, part):
    key_base, key_rows, key_cols = jax.random.split(jax.random.fold_in(key, 11), 3)
    column = jnp.arange(D, dtype=jnp.float32) / D
    shape_all = (MB, TOKENS_MB, D)
    base_values = jnp.clip(jax.random.normal(key_base, shape_all, jnp.float32), -3.5, 3.5)
    row_scale = jnp.exp(jax.random.uniform(key_rows, (MB, TOKENS_MB, 1), jnp.float32, jnp.log(0.3), jnp.log(3.0)))
    col_scale = jnp.exp(jnp.log(3.0) * column + jax.random.uniform(key_cols, (D,), jnp.float32, -0.35, 0.35))
    return (base_values * row_scale * col_scale).astype(jnp.bfloat16)


def level_of(stream_key, extent, pieces, smallest, high):
    loudness, own = 1.0, jax.random.fold_in(stream_key, 6)
    for dim, parts in pieces:
        heights = jnp.exp(jax.random.uniform(jax.random.fold_in(own, dim), (parts,), jnp.float32, smallest / len(pieces), high / len(pieces)))
        loudness = loudness * jnp.repeat(heights, extent[dim] // parts).reshape([-1 if axis == dim else 1 for axis in range(len(extent))])
    return loudness


def shared_out(stream_key, own, number, rows, amount, top, bound, slope):
    ranking = jax.random.permutation(stream_key, amount)
    crowded, usual = load_shares(amount, rows * top, bound, slope, True), load_shares(amount, rows * top, bound, slope, False)
    places = jnp.arange(amount)

    def named(sizes, turn):
        used = int((sizes > 0).sum())
        fixed = max(1, used // 4)
        moved = fixed + (places - fixed + turn * (used - fixed)) % max(1, amount - fixed)
        return jnp.zeros((amount,), jnp.int32).at[ranking[jnp.where(places < fixed, places, moved)]].set(jnp.asarray(sizes, jnp.int32))

    sizes = jnp.where(number % 4 == 0, named(crowded, number // 4), named(usual, number - number // 4 - 1))
    mixed = jax.random.permutation(jax.random.fold_in(own, 3), amount)
    donor, taker = mixed[0:amount // 2 * 2:2], mixed[1:amount // 2 * 2:2]
    margin = jnp.minimum(sizes[donor] - 1, bound - sizes[taker]) // 2
    margin = jnp.where((donor == ranking[0]) | (taker == ranking[0]) | (sizes[taker] == 0), 0, jnp.maximum(margin, 0))
    moved = jax.random.randint(jax.random.fold_in(own, 4), (amount // 2,), 0, 1 << 20) % (margin + 1)
    sizes = sizes.at[donor].add(-moved).at[taker].add(moved)
    labels = jnp.searchsorted(jnp.cumsum(sizes), jnp.arange(rows * top), side="right").astype(jnp.int32)
    grid = labels.reshape(top, rows).T
    grid = grid[jax.random.permutation(jax.random.fold_in(own, 1), rows)]
    turn = jax.random.randint(jax.random.fold_in(own, 2), (rows, 1), 0, top)
    return jnp.take_along_axis(grid, (jnp.arange(top)[None, :] + turn) % top, axis=1)


def load_shares(count, total, reach, slope, full):
    loads = [(1 << 20) // math.isqrt(grade ** slope) + 1 for grade in range(1, count + 1)]
    largest = reach if full else min(reach, max(-(-total // count), total * loads[0] // sum(loads)))
    least = 1 if total - largest >= count - 1 else 0
    counts, surplus = [largest] + [least] * (count - 1), total - largest - least * (count - 1)
    while surplus > 0:
        movable = [i for i in range(1, count) if counts[i] < largest] or [i for i in range(1, count) if counts[i] < reach]
        pool, budget = sum([loads[i] for i in movable]), surplus
        for i in movable:
            extra = min(reach - counts[i], max(1, budget * loads[i] // pool), surplus)
            counts[i] = counts[i] + extra
            surplus = surplus - extra
    return np.array(counts)


def normal_values(rng, shape, spread, bound, pieces=(), kind=jnp.bfloat16):
    factor_of = level_of(rng, shape, pieces, -0.22, 0.18) if pieces else 1.0
    result = jax.random.normal(rng, shape, jnp.float32) * spread * factor_of
    return jnp.minimum(jnp.maximum(result, -bound), bound).astype(kind)


def setup_inputs(seed: int = 0, part: int = 0) -> dict:
    keys = jax.random.split(jax.random.key(seed), 8)
    part_splits = jax.random.split(jax.random.fold_in(keys[7], part), 8)
    tokens = draw_tokens(jax.random.fold_in(jax.random.fold_in(keys[7], part), 71), part)
    route_ids_keys = jax.random.split(jax.random.fold_in(part_splits[1], 1), LAYERS * MB * TOKENS_MB // TOK_DEV)
    route_ids_turns = jax.random.permutation(jax.random.fold_in(part_splits[1], 3), LAYERS * MB * TOKENS_MB // TOK_DEV)
    route_ids = jax.vmap(lambda own, number: shared_out(jax.random.fold_in(part_splits[1], 2), own, number, TOK_DEV, EXPERTS, 2, CAP, 1))(route_ids_keys, route_ids_turns).reshape((LAYERS, MB, TOKENS_MB, 2))
    route_gates = jnp.clip(0.05 + 0.95 * jax.random.uniform(part_splits[2], (LAYERS, MB, TOKENS_MB, 2), jnp.float32) ** level_of(part_splits[2], (LAYERS, MB, TOKENS_MB, 2), ((2, 4),), -0.2, 0.2), 0.05, 1.0)
    norm_gain = jnp.clip(1.0 + 0.18 * jax.random.normal(keys[3], (LAYERS, D), jnp.float32), 0.1, 1.9)
    gate_weights = normal_values(keys[4], (LAYERS, D, EXPERTS * EXPERT_HIDDEN), D ** -0.5, 0.109375, ((1, 4), (2, 4)))
    up_weights = normal_values(keys[5], (LAYERS, D, EXPERTS * EXPERT_HIDDEN), D ** -0.5, 0.109375, ((1, 4), (2, 4)))
    down_weights = normal_values(keys[6], (LAYERS, EXPERTS * EXPERT_HIDDEN, D), EXPERT_HIDDEN ** -0.5, 0.0625, ((1, 4), (2, 4)))
    return {"tokens": tokens, "route_ids": route_ids, "route_gates": route_gates, "norm_gain": norm_gain, "gate_weights": gate_weights, "up_weights": up_weights, "down_weights": down_weights}


def expert_apply(packed):
    slot_rows, gate_matrix, up_matrix, down_weight = packed
    section_width = D // N_TENSOR
    block_units = EXPERT_HIDDEN // GROUP
    row_count = slot_rows.shape[0]
    section_count = slot_rows.reshape(row_count, N_TENSOR, section_width).astype(jnp.float32)
    gate_sections = jnp.einsum('ovk,vky->voy', section_count, gate_matrix.reshape(N_TENSOR, section_width, EXPERT_HIDDEN).astype(jnp.float32))
    up_sections = jnp.einsum('ovk,vky->voy', section_count, up_matrix.reshape(N_TENSOR, section_width, EXPERT_HIDDEN).astype(jnp.float32))
    gate_sections, up_sections = lax.optimization_barrier((gate_sections.astype(jnp.bfloat16), up_sections.astype(jnp.bfloat16)))
    gate_pre = lax.optimization_barrier(jnp.sum(gate_sections.astype(jnp.float32), axis=0))
    up_pre = lax.optimization_barrier(jnp.sum(up_sections.astype(jnp.float32), axis=0))
    hidden = (jax.nn.silu(gate_pre) * up_pre).astype(jnp.bfloat16)
    hidden_blocks = hidden.reshape(row_count, GROUP, block_units).astype(jnp.float32)
    down_blocks = down_weight.reshape(GROUP, block_units, D).astype(jnp.float32)
    down_parts = jnp.einsum('rbf,bfd->brd', hidden_blocks, down_blocks)
    down_parts = lax.optimization_barrier(down_parts.astype(jnp.bfloat16))
    return lax.optimization_barrier(jnp.sum(down_parts.astype(jnp.float32), axis=0))

def layer_apply(current, route_ids, route_gates, gain_row, gate_matrix, up_matrix, down_weight):
    values = current.astype(jnp.float32)
    squares = lax.optimization_barrier(jnp.sum(values * values, axis=1, keepdims=True))
    normed = (values * lax.rsqrt(squares / D + 1e-05) * gain_row).astype(jnp.bfloat16)
    flat_ids = route_ids.reshape(N_EXPERT, 2 * TOK_DEV).astype(jnp.int32)
    one_hot = (flat_ids[:, :, None] == jnp.arange(EXPERTS, dtype=jnp.int32)).astype(jnp.int32)
    earlier = jnp.cumsum(one_hot, axis=1) - one_hot
    position = lax.optimization_barrier(jnp.sum(earlier * one_hot, axis=2))
    source = jnp.arange(N_EXPERT, dtype=jnp.int32)[:, None]
    slot_index = ((flat_ids * N_EXPERT + source) * CAP + position).reshape(-1).astype(jnp.int32)
    route_rows = jnp.repeat(normed, 2, axis=0)
    buffer = jnp.zeros((EXPERTS * N_EXPERT * CAP, D), jnp.bfloat16).at[slot_index].set(route_rows)
    gate_stack = jnp.transpose(gate_matrix.reshape(D, EXPERTS, EXPERT_HIDDEN), (1, 0, 2))
    up_stack = jnp.transpose(up_matrix.reshape(D, EXPERTS, EXPERT_HIDDEN), (1, 0, 2))
    down_stack = down_weight.reshape(EXPERTS, EXPERT_HIDDEN, D)
    results = lax.map(expert_apply, (buffer.reshape(EXPERTS, N_EXPERT * CAP, D), gate_stack, up_stack, down_stack))
    picked = results.reshape(EXPERTS * N_EXPERT * CAP, D)[slot_index].reshape(TOKENS_MB, 2, D)
    mixture = lax.optimization_barrier(jnp.sum(picked * route_gates[:, :, None], axis=1))
    return (values + mixture).astype(jnp.bfloat16)

def reference(tokens, route_ids, route_gates, norm_gain, gate_weights, up_weights, down_weights):
    finished = []
    for batch_step in range(MB):
        current = tokens[batch_step]
        for layer_index in range(LAYERS):
            current = layer_apply(current, route_ids[layer_index, batch_step], route_gates[layer_index, batch_step], norm_gain[layer_index], gate_weights[layer_index], up_weights[layer_index], down_weights[layer_index])
        finished.append(current)
    return jnp.stack(finished)
```

```python
import functools

import jax
import jax.numpy as jnp
from jax import lax
from jax.experimental import pallas as pl
from jax.experimental.pallas import tpu as pltpu
from jax.sharding import PartitionSpec as P

EXPERTS = 4
MESH_ID = pl.DeviceIdType.MESH
F32 = jnp.float32
BF16 = jnp.bfloat16


def reversed_bits(value, bits):
    out = 0
    for k in range(bits):
        out = out * 2 + (value >> k) % 2
    return out


def kernel(
    cfg,
    tok_ref,
    ids_ref,
    gates_ref,
    gain_ref,
    wg_ref,
    wu_ref,
    wd_ref,
    out_ref,
    wg_buf,
    wu_buf,
    wd_buf,
    x_ref,
    disp,
    arrived,
    xin,
    sqs,
    scale,
    part,
    hid,
    acc,
    back,
    ret,
    *rest,
):
    layers, micro, tok, ranks, T, width, chunks, W, wq, cap, SR = cfg
    nb = T.bit_length() - 1
    rbufs = rest[:nb]
    abufs = rest[nb : 2 * nb - 1]
    wsem, d_send, d_recv, s_send, s_recv, b_send, b_recv, rs_send, rs_recv, ag_send, ag_recv = rest[2 * nb - 1 :]
    t = lax.axis_index("tensor")
    e = lax.axis_index("expert")
    sharing = ranks // EXPERTS
    rows = micro * tok
    R = ranks * micro * cap
    feature_count = width * T
    bits = [(t // (1 << k)) % 2 for k in range(nb)]
    partner = [t + (1 - 2 * bits[k]) * (1 << k) for k in range(nb)]
    s_me = sum(bits[k] * (T >> (k + 1)) for k in range(nb))

    def wg_copy(l, c):
        return pltpu.make_async_copy(
            wg_ref.at[l, :, pl.ds(pl.multiple_of(c * W, W), W)], wg_buf.at[c], wsem.at[0, c]
        )

    def wu_copy(l, c):
        return pltpu.make_async_copy(
            wu_ref.at[l, :, pl.ds(pl.multiple_of(c * W, W), W)], wu_buf.at[c], wsem.at[1, c]
        )

    def wd_copy(l, c):
        return pltpu.make_async_copy(
            wd_ref.at[l, pl.ds(pl.multiple_of(c * W, W), W), :], wd_buf.at[c], wsem.at[2, c]
        )

    def start_gu(c, _):
        wg_copy(0, c).start()
        wu_copy(0, c).start()
        return 0

    def start_d(c, _):
        wd_copy(0, c).start()
        return 0

    lax.fori_loop(0, chunks, start_gu, 0)
    lax.fori_loop(0, chunks, start_d, 0)

    barrier = pltpu.get_barrier_semaphore()
    for d in range(1, T):
        pl.semaphore_signal(barrier, inc=1, device_id={"tensor": (t + d) % T}, device_id_type=MESH_ID)
    for d in range(1, ranks):
        pl.semaphore_signal(barrier, inc=1, device_id={"expert": (e + d) % ranks}, device_id_type=MESH_ID)

    def disp_copy(l, d):
        peer = (e + d) % ranks
        return pltpu.make_async_remote_copy(
            src_ref=disp.at[l, peer // sharing],
            dst_ref=arrived.at[l, e],
            send_sem=d_send.at[l, d],
            recv_sem=d_recv.at[l, d],
            device_id={"expert": peer},
            device_id_type=MESH_ID,
        )

    def sq_copy(l, d):
        return pltpu.make_async_remote_copy(
            src_ref=sqs.at[l, t],
            dst_ref=sqs.at[l, t],
            send_sem=s_send.at[l, d],
            recv_sem=s_recv.at[l, d],
            device_id={"tensor": (t + d) % T},
            device_id_type=MESH_ID,
        )

    def back_copy(l, d):
        peer = (e + d) % ranks
        return pltpu.make_async_remote_copy(
            src_ref=back.at[l, peer],
            dst_ref=ret.at[l, e],
            send_sem=b_send.at[l, d],
            recv_sem=b_recv.at[l, d],
            device_id={"expert": peer},
            device_id_type=MESH_ID,
        )

    def rs_copy(l, c, k):
        half = T >> (k + 1)
        source = part if k == 0 else abufs[k - 1]
        return pltpu.make_async_remote_copy(
            src_ref=source.at[l, c, pl.ds((1 - bits[k]) * half, half)],
            dst_ref=rbufs[k].at[l, c],
            send_sem=rs_send.at[k, l, c],
            recv_sem=rs_recv.at[k, l, c],
            device_id={"tensor": partner[k]},
            device_id_type=MESH_ID,
        )

    def ag_copy(l, c, k):
        size = T >> (k + 1)
        base = sum(bits[i] * (T >> (i + 1)) for i in range(k + 1))
        block = hid.at[l, c, pl.ds(base, size)]
        return pltpu.make_async_remote_copy(
            src_ref=block,
            dst_ref=block,
            send_sem=ag_send.at[k, l, c],
            recv_sem=ag_recv.at[k, l, c],
            device_id={"tensor": partner[k]},
            device_id_type=MESH_ID,
        )

    x_ref[...] = tok_ref[...].astype(F32)

    dense = lax.broadcasted_iota(jnp.int32, (R, ranks * SR), 0)
    padded = lax.broadcasted_iota(jnp.int32, (R, ranks * SR), 1)
    place = padded & (SR - 1)
    shift = SR.bit_length() - 1
    pack = jnp.where(
        (dense == (padded >> shift) * (micro * cap) + place) & (place < micro * cap), 1.0, 0.0
    ).astype(BF16)

    row_i = lax.broadcasted_iota(jnp.int32, (rows, rows), 0)
    col_i = lax.broadcasted_iota(jnp.int32, (rows, rows), 1)
    same_micro = row_i >= 0
    for j in range(1, micro):
        same_micro = same_micro & ((row_i >= j * tok) == (col_i >= j * tok))
    own_micro = jnp.zeros((rows, 1), F32)
    row_one = lax.broadcasted_iota(jnp.int32, (rows, 1), 0)
    for j in range(1, micro):
        own_micro = own_micro + jnp.where(row_one >= j * tok, 1.0, 0.0)
    slot_iota = lax.broadcasted_iota(jnp.int32, (rows, EXPERTS * SR), 1).astype(F32)

    def slot_hits(l):
        ids = ids_ref[l].astype(F32)
        cols = [ids[:, 0:1], ids[:, 1:2]]
        across = [jnp.sum(jnp.where(row_i == col_i, c, 0.0), axis=0, keepdims=True) for c in cols]
        hits = []
        for k in range(2):
            position = jnp.zeros((rows, 1), F32)
            for other in range(2):
                before = (col_i <= row_i) if other < k else (col_i < row_i)
                match = (cols[k] == across[other]) & before & same_micro
                position = position + jnp.sum(jnp.where(match, 1.0, 0.0), axis=1, keepdims=True)
            slot = cols[k] * SR + own_micro * cap + position
            hits.append(jnp.where(slot == slot_iota, 1.0, 0.0))
        return hits

    lags = [1 if (k == 0 and T == 4) else 2 for k in range(nb)]
    rs_off = [sum(lags[: k + 1]) for k in range(nb)]
    ag_off, at = [0] * nb, rs_off[-1]
    for k in reversed(range(nb)):
        at += lags[k]
        ag_off[k] = at

    def layer(l, _):
        hits = slot_hits(l)
        picks = (hits[0] + hits[1]).astype(BF16)
        out_rows = lax.dot_general(
            picks, x_ref[...].astype(BF16), (((0,), (0,)), ((), ())), preferred_element_type=F32
        )
        disp[l] = out_rows.astype(BF16).reshape(EXPERTS, SR, width)

        @pl.when(l == 0)
        def _():
            pl.semaphore_wait(barrier, T + ranks - 2)

        for d in range(1, ranks):
            disp_copy(l, d).start()
        arrived[l, e] = disp[l, e // sharing]
        for d in range(1, ranks):
            disp_copy(l, d).wait_recv()
        got = jnp.dot(
            pack, arrived[l].reshape(ranks * SR, width), preferred_element_type=F32
        )
        squares = jnp.sum(got * got, axis=1, keepdims=True)
        sqs[l, t] = jnp.broadcast_to(squares, (R, 128))
        for d in range(1, T):
            sq_copy(l, d).start()
        xin[...] = (got * gain_ref[l]).astype(BF16)
        acc[...] = jnp.zeros_like(acc)

        def gate_up(c):
            wg_copy(l, c).wait()
            wu_copy(l, c).wait()
            for q in range(T):
                s = reversed_bits(q, nb)
                part[l, c, s, :, 0:wq] = jnp.dot(
                    xin[...], wg_buf[c, :, q * wq : (q + 1) * wq], preferred_element_type=F32
                ).astype(BF16)
                part[l, c, s, :, wq : 2 * wq] = jnp.dot(
                    xin[...], wu_buf[c, :, q * wq : (q + 1) * wq], preferred_element_type=F32
                ).astype(BF16)
            rs_copy(l, c, 0).start()

            @pl.when(l + 1 < layers)
            def _():
                wg_copy(l + 1, c).start()
                wu_copy(l + 1, c).start()

        def reduce(c, k):
            half = T >> (k + 1)
            rs_copy(l, c, k).wait_recv()
            source = part if k == 0 else abufs[k - 1]
            total = source[l, c, pl.ds(bits[k] * half, half)].astype(F32) + rbufs[k][l, c].astype(F32)
            if k < nb - 1:
                abufs[k][l, c] = total.astype(BF16)
                rs_copy(l, c, k + 1).start()
            else:
                factor = scale[:, 0:1]
                gate = total[0, :, 0:wq] * factor
                up = total[0, :, wq : 2 * wq] * factor
                hid[l, c, s_me] = (gate / (1.0 + jnp.exp(-gate)) * up).astype(BF16)
                ag_copy(l, c, nb - 1).start()

        def gather(c, k):
            ag_copy(l, c, k).wait_recv()
            if k > 0:
                ag_copy(l, c, k - 1).start()
            else:
                down(c)

        def down(c):
            wd_copy(l, c).wait()
            total = acc[...]
            for s in range(T):
                q = reversed_bits(s, nb)
                total = total + jnp.dot(
                    hid[l, c, s], wd_buf[c, q * wq : (q + 1) * wq, :], preferred_element_type=F32
                )
            acc[...] = total

            @pl.when(l + 1 < layers)
            def _():
                wd_copy(l + 1, c).start()

        def step(i, _):
            @pl.when(i < chunks)
            def _():
                gate_up(i)

            @pl.when(i == rs_off[-1])
            def _():
                for d in range(1, T):
                    sq_copy(l, d).wait_recv()
                total = sqs[l, 0]
                for j in range(1, T):
                    total = total + sqs[l, j]
                scale[...] = lax.rsqrt(total / feature_count + 1e-05)

            for k in range(nb):
                c = i - rs_off[k]
                pl.when((c >= 0) & (c < chunks))(functools.partial(reduce, c, k))
            for k in reversed(range(nb)):
                c = i - ag_off[k]
                pl.when((c >= 0) & (c < chunks))(functools.partial(gather, c, k))
            return 0

        lax.fori_loop(0, chunks + ag_off[0], step, 0)

        spread = lax.dot_general(
            pack, acc[...].astype(BF16), (((0,), (0,)), ((), ())), preferred_element_type=F32
        )
        back[l] = spread.astype(BF16).reshape(ranks, SR, width)
        for d in range(1, ranks):
            back_copy(l, d).start()
        ret[l, e] = back[l, e]
        gates = gates_ref[l]
        weights = hits[0] * gates[:, 0:1] + hits[1] * gates[:, 1:2]
        for d in range(1, ranks):
            back_copy(l, d).wait_recv()
        results = ret[l].astype(F32)
        if sharing > 1:
            results = jnp.sum(results.reshape(EXPERTS, sharing, SR, width), axis=1)
        mixture = jnp.dot(
            weights,
            results.reshape(EXPERTS * SR, width),
            preferred_element_type=F32,
            precision=lax.Precision.HIGHEST,
        )
        x_ref[...] = (x_ref[...] + mixture).astype(BF16).astype(F32)
        return 0

    lax.fori_loop(0, layers, layer, 0)
    out_ref[...] = x_ref[...].astype(BF16)

    def drain(l, _):
        for d in range(1, ranks):
            disp_copy(l, d).wait_send()
            back_copy(l, d).wait_send()
        for d in range(1, T):
            sq_copy(l, d).wait_send()

        def drain_chunk(c, _):
            for k in range(nb):
                rs_copy(l, c, k).wait_send()
                ag_copy(l, c, k).wait_send()
            return 0

        lax.fori_loop(0, chunks, drain_chunk, 0)
        return 0

    lax.fori_loop(0, layers, drain, 0)


def shards(ranks, T, tokens, route_ids, route_gates, norm_gain, gate_weights, up_weights, down_weights):
    micro, tok, width = tokens.shape
    layers = route_ids.shape[0]
    hidden = gate_weights.shape[2]
    rows = micro * tok
    cap = 3 * tok // 4
    SR = 16
    while SR < micro * cap:
        SR *= 2
    chunks = 8
    while chunks > 1 and hidden // chunks < 256 * T:
        chunks //= 2
    W = hidden // chunks
    wq = W // T
    nb = T.bit_length() - 1
    R = ranks * micro * cap
    cfg = (layers, micro, tok, ranks, T, width, chunks, W, wq, cap, SR)
    vmem = pl.BlockSpec(memory_space=pltpu.VMEM)
    hbm = pl.BlockSpec(memory_space=pl.ANY)
    dma = pltpu.SemaphoreType.DMA
    out = pl.pallas_call(
        functools.partial(kernel, cfg),
        out_shape=jax.ShapeDtypeStruct((rows, width), BF16),
        in_specs=[vmem] * 4 + [hbm] * 3,
        out_specs=vmem,
        scratch_shapes=[
            pltpu.VMEM((chunks, width, W), BF16),
            pltpu.VMEM((chunks, width, W), BF16),
            pltpu.VMEM((chunks, W, width), BF16),
            pltpu.VMEM((rows, width), F32),
            pltpu.VMEM((layers, EXPERTS, SR, width), BF16),
            pltpu.VMEM((layers, ranks, SR, width), BF16),
            pltpu.VMEM((R, width), BF16),
            pltpu.VMEM((layers, T, R, 128), F32),
            pltpu.VMEM((R, 128), F32),
            pltpu.VMEM((layers, chunks, T, R, 2 * wq), BF16),
            pltpu.VMEM((layers, chunks, T, R, wq), BF16),
            pltpu.VMEM((R, width), F32),
            pltpu.VMEM((layers, ranks, SR, width), BF16),
            pltpu.VMEM((layers, ranks, SR, width), BF16),
        ]
        + [pltpu.VMEM((layers, chunks, T >> (k + 1), R, 2 * wq), BF16) for k in range(nb)]
        + [pltpu.VMEM((layers, chunks, T >> (k + 1), R, 2 * wq), BF16) for k in range(nb - 1)]
        + [
            dma((3, chunks)),
            dma((layers, ranks)),
            dma((layers, ranks)),
            dma((layers, T)),
            dma((layers, T)),
            dma((layers, ranks)),
            dma((layers, ranks)),
            dma((nb, layers, chunks)),
            dma((nb, layers, chunks)),
            dma((nb, layers, chunks)),
            dma((nb, layers, chunks)),
        ],
        compiler_params=pltpu.CompilerParams(
            collective_id=0, has_side_effects=True, vmem_limit_bytes=64 * 1024 * 1024 - 65536
        ),
    )(
        tokens.reshape(rows, width),
        route_ids.reshape(layers, rows, 2),
        route_gates.reshape(layers, rows, 2),
        norm_gain.reshape(layers, 1, width),
        gate_weights,
        up_weights,
        down_weights,
    )
    return out.reshape(micro, tok, width)


def solution(mesh):
    in_specs = (
        P(None, ("groups", "expert"), "tensor"),
        P(None, None, ("groups", "expert"), None),
        P(None, None, ("groups", "expert"), None),
        P(None, "tensor"),
        P(None, "tensor", "expert"),
        P(None, "tensor", "expert"),
        P(None, "expert", "tensor"),
    )
    out_specs = P(None, ("groups", "expert"), "tensor")
    body = functools.partial(shards, mesh.shape["expert"], mesh.shape["tensor"])
    return jax.shard_map(body, mesh=mesh, in_specs=in_specs, out_specs=out_specs, check_vma=False)
```

```python
import functools

import jax
import jax.numpy as jnp
from jax import lax
from jax.experimental import pallas as pl
from jax.experimental.pallas import tpu as pltpu
from jax.sharding import PartitionSpec as P

EXPERTS = 4
MESH_ID = pl.DeviceIdType.MESH
F32 = jnp.float32
BF16 = jnp.bfloat16


def reversed_bits(value, bits):
    out = 0
    for k in range(bits):
        out = out * 2 + (value >> k) % 2
    return out


def kernel(
    cfg,
    tok_ref,
    ids_ref,
    gates_ref,
    gain_ref,
    wg_ref,
    wu_ref,
    wd_ref,
    out_ref,
    wg_buf,
    wu_buf,
    wd_buf,
    x_ref,
    disp,
    arrived,
    xin,
    sqs,
    scale,
    part,
    hid,
    acc,
    back,
    ret,
    *rest,
):
    layers, micro, tok, ranks, T, width, chunks, W, wq, cap, SR = cfg
    nb = T.bit_length() - 1
    rbufs = rest[:nb]
    abufs = rest[nb : 2 * nb - 1]
    wsem, d_send, d_recv, s_send, s_recv, b_send, b_recv, rs_send, rs_recv, ag_send, ag_recv = rest[2 * nb - 1 :]
    t = lax.axis_index("tensor")
    e = lax.axis_index("expert")
    sharing = ranks // EXPERTS
    rows = micro * tok
    R = ranks * micro * cap
    feature_count = width * T
    bits = [(t // (1 << k)) % 2 for k in range(nb)]
    partner = [t + (1 - 2 * bits[k]) * (1 << k) for k in range(nb)]
    s_me = sum(bits[k] * (T >> (k + 1)) for k in range(nb))

    def wg_copy(l, c):
        return pltpu.make_async_copy(
            wg_ref.at[l, :, pl.ds(pl.multiple_of(c * W, W), W)], wg_buf.at[c], wsem.at[0, c]
        )

    def wu_copy(l, c):
        return pltpu.make_async_copy(
            wu_ref.at[l, :, pl.ds(pl.multiple_of(c * W, W), W)], wu_buf.at[c], wsem.at[1, c]
        )

    def wd_copy(l, c):
        return pltpu.make_async_copy(
            wd_ref.at[l, pl.ds(pl.multiple_of(c * W, W), W), :], wd_buf.at[c], wsem.at[2, c]
        )

    def start_gu(c, _):
        wg_copy(0, c).start()
        wu_copy(0, c).start()
        return 0

    def start_d(c, _):
        wd_copy(0, c).start()
        return 0

    lax.fori_loop(0, chunks, start_gu, 0)
    lax.fori_loop(0, chunks, start_d, 0)

    barrier = pltpu.get_barrier_semaphore()
    for d in range(1, T):
        pl.semaphore_signal(barrier, inc=1, device_id={"tensor": (t + d) % T}, device_id_type=MESH_ID)
    for d in range(1, ranks):
        pl.semaphore_signal(barrier, inc=1, device_id={"expert": (e + d) % ranks}, device_id_type=MESH_ID)

    def disp_copy(l, d):
        peer = (e + d) % ranks
        return pltpu.make_async_remote_copy(
            src_ref=disp.at[l, peer // sharing],
            dst_ref=arrived.at[l, e],
            send_sem=d_send.at[l, d],
            recv_sem=d_recv.at[l, d],
            device_id={"expert": peer},
            device_id_type=MESH_ID,
        )

    def sq_copy(l, d):
        return pltpu.make_async_remote_copy(
            src_ref=sqs.at[l, t],
            dst_ref=sqs.at[l, t],
            send_sem=s_send.at[l, d],
            recv_sem=s_recv.at[l, d],
            device_id={"tensor": (t + d) % T},
            device_id_type=MESH_ID,
        )

    def back_copy(l, d):
        peer = (e + d) % ranks
        return pltpu.make_async_remote_copy(
            src_ref=back.at[l, peer],
            dst_ref=ret.at[l, e],
            send_sem=b_send.at[l, d],
            recv_sem=b_recv.at[l, d],
            device_id={"expert": peer},
            device_id_type=MESH_ID,
        )

    def rs_copy(l, c, k):
        half = T >> (k + 1)
        source = part if k == 0 else abufs[k - 1]
        return pltpu.make_async_remote_copy(
            src_ref=source.at[l, c, pl.ds((1 - bits[k]) * half, half)],
            dst_ref=rbufs[k].at[l, c],
            send_sem=rs_send.at[k, l, c],
            recv_sem=rs_recv.at[k, l, c],
            device_id={"tensor": partner[k]},
            device_id_type=MESH_ID,
        )

    def ag_copy(l, c, k):
        size = T >> (k + 1)
        base = sum(bits[i] * (T >> (i + 1)) for i in range(k + 1))
        block = hid.at[l, c, pl.ds(base, size)]
        return pltpu.make_async_remote_copy(
            src_ref=block,
            dst_ref=block,
            send_sem=ag_send.at[k, l, c],
            recv_sem=ag_recv.at[k, l, c],
            device_id={"tensor": partner[k]},
            device_id_type=MESH_ID,
        )

    x_ref[...] = tok_ref[...].astype(F32)

    dense = lax.broadcasted_iota(jnp.int32, (R, ranks * SR), 0)
    padded = lax.broadcasted_iota(jnp.int32, (R, ranks * SR), 1)
    place = padded & (SR - 1)
    shift = SR.bit_length() - 1
    pack = jnp.where(
        (dense == (padded >> shift) * (micro * cap) + place) & (place < micro * cap), 1.0, 0.0
    ).astype(BF16)

    row_i = lax.broadcasted_iota(jnp.int32, (rows, rows), 0)
    col_i = lax.broadcasted_iota(jnp.int32, (rows, rows), 1)
    same_micro = row_i >= 0
    for j in range(1, micro):
        same_micro = same_micro & ((row_i >= j * tok) == (col_i >= j * tok))
    own_micro = jnp.zeros((rows, 1), F32)
    row_one = lax.broadcasted_iota(jnp.int32, (rows, 1), 0)
    for j in range(1, micro):
        own_micro = own_micro + jnp.where(row_one >= j * tok, 1.0, 0.0)
    slot_iota = lax.broadcasted_iota(jnp.int32, (rows, EXPERTS * SR), 1).astype(F32)

    def slot_hits(l):
        ids = ids_ref[l].astype(F32)
        cols = [ids[:, 0:1], ids[:, 1:2]]
        across = [jnp.sum(jnp.where(row_i == col_i, c, 0.0), axis=0, keepdims=True) for c in cols]
        hits = []
        for k in range(2):
            position = jnp.zeros((rows, 1), F32)
            for other in range(2):
                before = (col_i <= row_i) if other < k else (col_i < row_i)
                match = (cols[k] == across[other]) & before & same_micro
                position = position + jnp.sum(jnp.where(match, 1.0, 0.0), axis=1, keepdims=True)
            slot = cols[k] * SR + own_micro * cap + position
            hits.append(jnp.where(slot == slot_iota, 1.0, 0.0))
        return hits

    lags = [1 if (k == 0 and T == 4) else 3 for k in range(nb)]
    rs_off = [sum(lags[: k + 1]) for k in range(nb)]
    ag_off, at = [0] * nb, rs_off[-1]
    for k in reversed(range(nb)):
        at += lags[k]
        ag_off[k] = at

    def layer(l, _):
        hits = slot_hits(l)
        picks = (hits[0] + hits[1]).astype(BF16)
        out_rows = lax.dot_general(
            picks, x_ref[...].astype(BF16), (((0,), (0,)), ((), ())), preferred_element_type=F32
        )
        disp[l] = out_rows.astype(BF16).reshape(EXPERTS, SR, width)

        @pl.when(l == 0)
        def _():
            pl.semaphore_wait(barrier, T + ranks - 2)

        for d in range(1, ranks):
            disp_copy(l, d).start()
        arrived[l, e] = disp[l, e // sharing]
        for d in range(1, ranks):
            disp_copy(l, d).wait_recv()
        got = jnp.dot(
            pack, arrived[l].reshape(ranks * SR, width), preferred_element_type=F32
        )
        squares = jnp.sum(got * got, axis=1, keepdims=True)
        sqs[l, t] = jnp.broadcast_to(squares, (R, 128))
        for d in range(1, T):
            sq_copy(l, d).start()
        xin[...] = (got * gain_ref[l]).astype(BF16)
        acc[...] = jnp.zeros_like(acc)

        def gate_up(c):
            wg_copy(l, c).wait()
            wu_copy(l, c).wait()
            for q in range(T):
                s = reversed_bits(q, nb)
                part[l, c, s, :, 0:wq] = jnp.dot(
                    xin[...], wg_buf[c, :, q * wq : (q + 1) * wq], preferred_element_type=F32
                ).astype(BF16)
                part[l, c, s, :, wq : 2 * wq] = jnp.dot(
                    xin[...], wu_buf[c, :, q * wq : (q + 1) * wq], preferred_element_type=F32
                ).astype(BF16)
            rs_copy(l, c, 0).start()

            @pl.when(l + 1 < layers)
            def _():
                wg_copy(l + 1, c).start()
                wu_copy(l + 1, c).start()

        def reduce(c, k):
            half = T >> (k + 1)
            rs_copy(l, c, k).wait_recv()
            source = part if k == 0 else abufs[k - 1]
            total = source[l, c, pl.ds(bits[k] * half, half)].astype(F32) + rbufs[k][l, c].astype(F32)
            if k < nb - 1:
                abufs[k][l, c] = total.astype(BF16)
                rs_copy(l, c, k + 1).start()
            else:
                factor = scale[:, 0:1]
                gate = total[0, :, 0:wq] * factor
                up = total[0, :, wq : 2 * wq] * factor
                hid[l, c, s_me] = (gate / (1.0 + jnp.exp(-gate)) * up).astype(BF16)
                ag_copy(l, c, nb - 1).start()

        def gather(c, k):
            ag_copy(l, c, k).wait_recv()
            if k > 0:
                ag_copy(l, c, k - 1).start()
            else:
                down(c)

        def down(c):
            wd_copy(l, c).wait()
            total = acc[...]
            for s in range(T):
                q = reversed_bits(s, nb)
                total = total + jnp.dot(
                    hid[l, c, s], wd_buf[c, q * wq : (q + 1) * wq, :], preferred_element_type=F32
                )
            acc[...] = total

            @pl.when(l + 1 < layers)
            def _():
                wd_copy(l + 1, c).start()

        def step(i, _):
            @pl.when(i < chunks)
            def _():
                gate_up(i)

            @pl.when(i == rs_off[-1])
            def _():
                for d in range(1, T):
                    sq_copy(l, d).wait_recv()
                total = sqs[l, 0]
                for j in range(1, T):
                    total = total + sqs[l, j]
                scale[...] = lax.rsqrt(total / feature_count + 1e-05)

            for k in range(nb):
                c = i - rs_off[k]
                pl.when((c >= 0) & (c < chunks))(functools.partial(reduce, c, k))
            for k in reversed(range(nb)):
                c = i - ag_off[k]
                pl.when((c >= 0) & (c < chunks))(functools.partial(gather, c, k))
            return 0

        lax.fori_loop(0, chunks + ag_off[0], step, 0)

        spread = lax.dot_general(
            pack, acc[...].astype(BF16), (((0,), (0,)), ((), ())), preferred_element_type=F32
        )
        back[l] = spread.astype(BF16).reshape(ranks, SR, width)
        for d in range(1, ranks):
            back_copy(l, d).start()
        ret[l, e] = back[l, e]
        gates = gates_ref[l]
        weights = hits[0] * gates[:, 0:1] + hits[1] * gates[:, 1:2]
        for d in range(1, ranks):
            back_copy(l, d).wait_recv()
        results = ret[l].astype(F32)
        if sharing > 1:
            results = jnp.sum(results.reshape(EXPERTS, sharing, SR, width), axis=1)
        mixture = jnp.dot(
            weights,
            results.reshape(EXPERTS * SR, width),
            preferred_element_type=F32,
            precision=lax.Precision.HIGHEST,
        )
        x_ref[...] = (x_ref[...] + mixture).astype(BF16).astype(F32)
        return 0

    lax.fori_loop(0, layers, layer, 0)
    out_ref[...] = x_ref[...].astype(BF16)

    def drain(l, _):
        for d in range(1, ranks):
            disp_copy(l, d).wait_send()
            back_copy(l, d).wait_send()
        for d in range(1, T):
            sq_copy(l, d).wait_send()

        def drain_chunk(c, _):
            for k in range(nb):
                rs_copy(l, c, k).wait_send()
                ag_copy(l, c, k).wait_send()
            return 0

        lax.fori_loop(0, chunks, drain_chunk, 0)
        return 0

    lax.fori_loop(0, layers, drain, 0)


def shards(ranks, T, tokens, route_ids, route_gates, norm_gain, gate_weights, up_weights, down_weights):
    micro, tok, width = tokens.shape
    layers = route_ids.shape[0]
    hidden = gate_weights.shape[2]
    rows = micro * tok
    cap = 3 * tok // 4
    SR = 16
    while SR < micro * cap:
        SR *= 2
    chunks = 8
    while chunks > 1 and hidden // chunks < 256 * T:
        chunks //= 2
    W = hidden // chunks
    wq = W // T
    nb = T.bit_length() - 1
    R = ranks * micro * cap
    cfg = (layers, micro, tok, ranks, T, width, chunks, W, wq, cap, SR)
    vmem = pl.BlockSpec(memory_space=pltpu.VMEM)
    hbm = pl.BlockSpec(memory_space=pl.ANY)
    dma = pltpu.SemaphoreType.DMA
    out = pl.pallas_call(
        functools.partial(kernel, cfg),
        out_shape=jax.ShapeDtypeStruct((rows, width), BF16),
        in_specs=[vmem] * 4 + [hbm] * 3,
        out_specs=vmem,
        scratch_shapes=[
            pltpu.VMEM((chunks, width, W), BF16),
            pltpu.VMEM((chunks, width, W), BF16),
            pltpu.VMEM((chunks, W, width), BF16),
            pltpu.VMEM((rows, width), F32),
            pltpu.VMEM((layers, EXPERTS, SR, width), BF16),
            pltpu.VMEM((layers, ranks, SR, width), BF16),
            pltpu.VMEM((R, width), BF16),
            pltpu.VMEM((layers, T, R, 128), F32),
            pltpu.VMEM((R, 128), F32),
            pltpu.VMEM((layers, chunks, T, R, 2 * wq), BF16),
            pltpu.VMEM((layers, chunks, T, R, wq), BF16),
            pltpu.VMEM((R, width), F32),
            pltpu.VMEM((layers, ranks, SR, width), BF16),
            pltpu.VMEM((layers, ranks, SR, width), BF16),
        ]
        + [pltpu.VMEM((layers, chunks, T >> (k + 1), R, 2 * wq), BF16) for k in range(nb)]
        + [pltpu.VMEM((layers, chunks, T >> (k + 1), R, 2 * wq), BF16) for k in range(nb - 1)]
        + [
            dma((3, chunks)),
            dma((layers, ranks)),
            dma((layers, ranks)),
            dma((layers, T)),
            dma((layers, T)),
            dma((layers, ranks)),
            dma((layers, ranks)),
            dma((nb, layers, chunks)),
            dma((nb, layers, chunks)),
            dma((nb, layers, chunks)),
            dma((nb, layers, chunks)),
        ],
        compiler_params=pltpu.CompilerParams(
            collective_id=0, has_side_effects=True, vmem_limit_bytes=64 * 1024 * 1024 - 65536
        ),
    )(
        tokens.reshape(rows, width),
        route_ids.reshape(layers, rows, 2),
        route_gates.reshape(layers, rows, 2),
        norm_gain.reshape(layers, 1, width),
        gate_weights,
        up_weights,
        down_weights,
    )
    return out.reshape(micro, tok, width)


def solution(mesh):
    in_specs = (
        P(None, ("groups", "expert"), "tensor"),
        P(None, None, ("groups", "expert"), None),
        P(None, None, ("groups", "expert"), None),
        P(None, "tensor"),
        P(None, "tensor", "expert"),
        P(None, "tensor", "expert"),
        P(None, "expert", "tensor"),
    )
    out_specs = P(None, ("groups", "expert"), "tensor")
    body = functools.partial(shards, mesh.shape["expert"], mesh.shape["tensor"])
    return jax.shard_map(body, mesh=mesh, in_specs=in_specs, out_specs=out_specs, check_vma=False)
```
